32 devices in a mesh: rows: 8 (over z, y), cols: 4 (over x, core).
Axes of the slice: x: 2, y: 2, z: 4, core: 2. Of those that a mesh axis runs over, the one named last changes fastest.
Arguments:
- slab: float32 [1536, 6144], P('rows', 'cols'), may hold values from -6 to 6
- factor: float32 [6144, 6144], P('cols', 'rows'), may hold values from -0.078125 to 0.078125
- block_inverse: float32 [6144, 1536], P('cols'), may hold values from -2 to 2, as said below
- pivot_order: int32 [6144], replicated, may hold values from 0 to 6143, as said below
- row_count: int32 [8], P('rows'), may hold values from 1 to 192, 1075 in all
Outputs:
- vectors: float32 [1536, 6144], P('rows', 'cols')
- mean_square: float32 [1536], P('rows')
The draws below stay inside these ranges and needn't reach their ends.
Inputs may be any that keep to these rules, and one draw needn't show every extreme that they name: `pivot_order`: each of 0 to 6143 appears once. Of the 1536 pivots of one block, at most 768 have slab columns in any one block of 1536 slab columns, and exactly 768 in some. `row_count`: slots at or beyond the count hold entries that are ignored. `block_inverse`: each block of 1536 rows is lower triangular, with diagonal entries from 0.6 to 1.4.
All inputs are finite; a program needn't handle non-finite values. No bound on the sum of `row_count` on one device may be relied on, other than what follows from the above.
Results may differ from the reference program's by a relative error of at most 0.0001.
Values sent between devices are 32-bit elements; how exact they have to be, the bound alone decides.
A program may use at most 192 MiB of HBM per device.

```python
import math
import jax
import jax.numpy as jnp
import numpy as np
from jax import lax

K = 6144
ROWS_DEV = 192
BLOCK = 1536
ROWS = 1536
N_ROWS = 8
N_COLS = 4


def draw_block_inverse(key, part):
    first_key, second_key = jax.random.split(key)
    local_rows = jnp.arange(K, dtype=jnp.int32) % BLOCK
    local_cols = jnp.arange(BLOCK, dtype=jnp.int32)
    spread = jnp.clip(jax.random.normal(first_key, (K, BLOCK), jnp.float32), -4.0, 4.0)
    spread = spread / jnp.sqrt(jnp.float32(BLOCK))
    diagonal = jax.random.uniform(second_key, (K, 1), jnp.float32, 0.6, 1.4)
    lower = jnp.where(local_cols[None, :] < local_rows[:, None], spread, jnp.float32(0.0))
    return lower + jnp.where(local_cols[None, :] == local_rows[:, None], diagonal, jnp.float32(0.0))


def draw_pivot_order(key, part):
    keys = jax.random.split(jax.random.fold_in(key, 17), 4)
    group_count = K // BLOCK
    base = BLOCK // group_count
    shift = jax.random.randint(keys[0], (), 0, group_count, dtype=jnp.int32)
    extra = jax.random.randint(keys[1], (), 0, base // 2 + 1, dtype=jnp.int32)
    source = jnp.arange(group_count, dtype=jnp.int32)[:, None]
    target = jnp.arange(group_count, dtype=jnp.int32)[None, :]
    offset = (target - source - shift) % group_count
    counts = base + base * (offset == 0).astype(jnp.int32) - base * (offset == 1).astype(jnp.int32)
    counts = counts + extra * (offset == 2).astype(jnp.int32) - extra * (offset == 3).astype(jnp.int32)
    inclusive = jnp.cumsum(counts, axis=1)
    columns = jnp.arange(K, dtype=jnp.int32)
    column_block = columns // BLOCK
    first_perm = jax.random.permutation(keys[2], K).astype(jnp.int32)
    order = jnp.argsort(column_block * K + first_perm).astype(jnp.int32)
    position = jnp.argsort(order).astype(jnp.int32)
    local_rank = position - column_block * BLOCK
    bounds = jnp.take(inclusive, column_block, axis=0)
    destination = jnp.sum((bounds <= local_rank[:, None]).astype(jnp.int32), axis=1)
    second_perm = jax.random.permutation(keys[3], K).astype(jnp.int32)
    return jnp.argsort(destination * K + second_perm).astype(jnp.int32)


def block_levels(own_key, shape, cuts, least, high):
    def one(axis_at, blocks):
        steps = jax.random.uniform(jax.random.fold_in(jax.random.fold_in(own_key, 6), axis_at), (blocks,), jnp.float32, least / len(cuts), high / len(cuts))
        return jnp.repeat(jnp.exp(steps), shape[axis_at] // blocks).reshape((-1,) + (1,) * (len(shape) - axis_at - 1))

    factor_of = one(*cuts[0])
    for cut in cuts[1:]:
        factor_of = factor_of * one(*cut)
    return factor_of


def length_profile(number_of, total, most, lean):
    loads = [(1 << 20) // math.isqrt(rank ** lean) + 1 for rank in range(2, number_of + 1)]
    surplus, holding = total - most - (number_of - 1), [1] * (number_of - 1)
    while surplus > 0:
        candidates = [i for i in range(number_of - 1) if holding[i] < most]
        mass, remaining = sum([loads[i] for i in candidates]), surplus
        for i in candidates:
            addition = min(most - holding[i], max(1, remaining * loads[i] // mass), surplus)
            holding[i] = holding[i] + addition
            surplus = surplus - addition
    return np.array([most] + holding)


def uneven(stream_key, amount, total, limit, slope):
    if amount == 2:
        one = jax.random.randint(stream_key, (), max(1, total - limit), min(limit, total - 1) + 1)
        return jnp.stack([one, total - one])
    sizes = jnp.asarray(length_profile(amount, total, limit, slope), jnp.int32)
    couples = (amount - 1) // 2
    giver, sink = sizes[1:1 + 2 * couples:2], sizes[2:2 + 2 * couples:2]
    margin = jnp.minimum(giver - 1, limit - sink)
    passed = jax.random.randint(jax.random.fold_in(stream_key, 1), (couples,), 0, 1 << 20) % (margin + 1)
    sizes = sizes.at[1:1 + 2 * couples:2].set(giver - passed).at[2:2 + 2 * couples:2].set(sink + passed)
    return sizes[jax.random.permutation(jax.random.fold_in(stream_key, 2), amount)]


def scatter_about(rng, shape, scale, bound, shards=(), held_as=jnp.bfloat16):
    gain = block_levels(rng, shape, shards, -0.22, 0.18) if shards else 1.0
    drawn = jax.random.normal(rng, shape, jnp.float32) * scale * gain
    return jnp.minimum(jnp.maximum(drawn, -bound), bound).astype(held_as)


def setup_inputs(seed: int = 0) -> dict:
    key_list = jax.random.split(jax.random.key(seed), 6)
    slab = scatter_about(key_list[0], (ROWS, K), 1.0, 6.0, ((0, 8), (1, 4)), jnp.float32)
    factor = scatter_about(key_list[1], (K, K), K ** -0.5, 0.078125, ((0, 4), (1, 8)), jnp.float32)
    block_inverse = draw_block_inverse(jax.random.fold_in(key_list[5], 71), 0)
    pivot_order = draw_pivot_order(jax.random.fold_in(key_list[5], 71), 0)
    row_count = uneven(key_list[4], N_ROWS, (7 * ROWS) // 10, ROWS_DEV, 2).astype(jnp.int32)
    return dict(slab=slab, factor=factor, block_inverse=block_inverse, pivot_order=pivot_order, row_count=row_count)


def reference(slab, factor, block_inverse, pivot_order, row_count):
    ordered = jnp.take(slab, pivot_order, axis=1)
    slot_index = jnp.arange(ROWS, dtype=jnp.int32) % ROWS_DEV
    owner = jnp.arange(ROWS, dtype=jnp.int32) // ROWS_DEV
    live_rows = slot_index < row_count[owner]
    ordered = jnp.where(live_rows[:, None], ordered, jnp.float32(0.0))
    block_width = K // N_COLS
    finished = []
    for column_block in range(N_COLS):
        low = column_block * block_width
        remainder = ordered[:, low:low + block_width]
        for earlier in range(column_block):
            weights = factor[low:low + block_width, earlier * block_width:(earlier + 1) * block_width]
            remainder = remainder - jnp.dot(finished[earlier], weights.T, precision=lax.Precision.HIGHEST, preferred_element_type=jnp.float32)
        inverse = block_inverse[low:low + block_width]
        finished.append(jnp.dot(remainder, inverse.T, precision=lax.Precision.HIGHEST, preferred_element_type=jnp.float32))
    vectors = jnp.concatenate(finished, axis=1)
    mean_square = jnp.sum(vectors * vectors, axis=1) / K
    return vectors, mean_square
```

```python
import functools
import jax
import jax.numpy as jnp
from jax import lax
from jax.experimental import pallas as pl
from jax.experimental.pallas import tpu as pltpu
from jax.sharding import PartitionSpec as P

MESH = pl.DeviceIdType.MESH


def times_transposed(left, right):
    return lax.dot_general(
        left,
        right,
        (((1,), (1,)), ((), ())),
        precision=lax.Precision.HIGH,
        preferred_element_type=jnp.float32,
    )


def gather_kernel(groups, side, chunks, part_ref, row_ref, mine, in_sem, keep_sem, right_sem, left_sem, hop_sem, side_sem, cross_sem):
    row, column = lax.axis_index("rows"), lax.axis_index("cols")
    a, b = row // side, row % side
    depth, width = part_ref.shape
    tall = depth // chunks

    def at(a_to, b_to):
        return (a_to * side + b_to, column)

    barrier = pltpu.get_barrier_semaphore()
    for step in (1, groups - 1):
        pl.semaphore_signal(barrier, inc=1, device_id=at((a + step) % groups, b), device_id_type=MESH)
    for step in range(1, side):
        pl.semaphore_signal(barrier, inc=1, device_id=at(a, (b + step) % side), device_id_type=MESH)
    pl.semaphore_wait(barrier, 2 + side - 1)

    def rows_of(i):
        return pl.ds(pl.multiple_of(i * tall, tall), tall)

    def place(k, b_of, i):
        return row_ref.at[k * side + b_of, rows_of(i), :]

    def right(k, i, source):
        return pltpu.make_async_remote_copy(source, place(k, b, i), right_sem.at[k, i], hop_sem.at[k, i], device_id=at(jnp.minimum(a + 1, groups - 1), b), device_id_type=MESH)

    def left(k, i, source):
        return pltpu.make_async_remote_copy(source, place(k, b, i), left_sem.at[k, i], hop_sem.at[k, i], device_id=at(jnp.maximum(a - 1, 0), b), device_id_type=MESH)

    def across(k, step, i, source):
        return pltpu.make_async_remote_copy(source, place(k, b, i), side_sem.at[step - 1, k, i], cross_sem.at[step - 1, k, i], device_id=at(a, (b + step) % side), device_id_type=MESH)

    def load(i):
        return pltpu.make_async_copy(part_ref.at[rows_of(i), :], mine.at[rows_of(i), :], in_sem.at[i])

    def keep(i):
        return pltpu.make_async_copy(mine.at[rows_of(i), :], place(a, b, i), keep_sem.at[i])

    @pl.when(a < column)
    def _():
        @pl.loop(0, chunks)
        def _(i):
            load(i).start()

        @pl.loop(0, chunks)
        def _(i):
            source = mine.at[rows_of(i), :]
            load(i).wait()

            @pl.when(a < groups - 1)
            def _():
                right(a, i, source).start()

            @pl.when(a > 0)
            def _():
                left(a, i, source).start()

            for step in range(1, side):
                across(a, step, i, source).start()
            keep(i).start()

    for hop in range(1, groups):
        @pl.loop(0, chunks)
        def _(i):
            k = a - hop

            @pl.when((k >= 0) & (k < column))
            def _():
                source = place(k, b, i)
                right(k, i, source).wait_recv()

                @pl.when(a < groups - 1)
                def _():
                    right(k, i, source).start()

                for step in range(1, side):
                    across(k, step, i, source).start()

            h = a + hop

            @pl.when((h <= groups - 1) & (h < column))
            def _():
                source = place(h, b, i)
                left(h, i, source).wait_recv()

                @pl.when(a > 0)
                def _():
                    left(h, i, source).start()

                for step in range(1, side):
                    across(h, step, i, source).start()

    for k in range(groups - 1):
        @pl.when(k < column)
        def _():
            @pl.loop(0, chunks)
            def _(i):
                source = place(k, b, i)
                for step in range(1, side):
                    came = place(k, (b + side - step) % side, i)
                    pltpu.make_async_remote_copy(came, came, side_sem.at[step - 1, k, i], cross_sem.at[step - 1, k, i], device_id=at(a, (b + step) % side), device_id_type=MESH).wait_recv()
                    across(k, step, i, source).wait_send()

                @pl.when((k <= a) & (a < groups - 1))
                def _():
                    right(k, i, source).wait_send()

                @pl.when((k >= a) & (a > 0))
                def _():
                    left(k, i, source).wait_send()

                @pl.when(k == a)
                def _():
                    keep(i).wait()


def gather_factor(factor, rows, groups):
    side = rows // groups
    depth, width = factor.shape
    chunks = max(1, depth // 256)
    sem = pltpu.SemaphoreType.DMA
    return pl.pallas_call(
        functools.partial(gather_kernel, groups, side, chunks),
        out_shape=jax.ShapeDtypeStruct(((groups - 1) * side, depth, width), jnp.float32),
        in_specs=[pl.BlockSpec(memory_space=pl.ANY)],
        out_specs=pl.BlockSpec(memory_space=pl.ANY),
        scratch_shapes=[
            pltpu.VMEM((depth, width), jnp.float32),
            sem((chunks,)),
            sem((chunks,)),
            sem((groups, chunks)),
            sem((groups, chunks)),
            sem((groups, chunks)),
            sem((side - 1, groups, chunks)),
            sem((side - 1, groups, chunks)),
        ],
        compiler_params=pltpu.CompilerParams(collective_id=0, has_side_effects=True, vmem_limit_bytes=60000 * 1024),
        cost_estimate=pl.CostEstimate(flops=0, bytes_accessed=600000000, transcendentals=0),
    )(factor)


def per_device(slab, factor, block_inverse, pivot_order, row_count):
    rows_here, block_width = slab.shape
    row_devices = lax.axis_size("rows")
    column_count = lax.axis_size("cols")
    column = lax.axis_index("cols")
    total_width = block_width * column_count
    side = row_devices // column_count
    chosen = lax.dynamic_slice_in_dim(pivot_order, column * block_width, block_width)
    gathered = lax.all_gather(slab, "cols", axis=1, tiled=True)
    parts = gather_factor(factor, row_devices, column_count)
    gathered, parts = lax.optimization_barrier((gathered, parts))
    ordered = jnp.take(gathered, chosen, axis=1)
    live_rows = jnp.arange(rows_here, dtype=jnp.int32) < row_count[0]
    pending = jnp.where(live_rows[:, None], ordered, jnp.float32(0.0))

    def finish(values):
        return times_transposed(values, block_inverse)

    def nothing(values):
        return jnp.zeros_like(values)

    width = factor.shape[1]
    vectors = jnp.zeros_like(pending)
    for k in range(column_count):
        finished = lax.cond(column == k, finish, nothing, pending)
        vectors = vectors + finished
        if k + 1 < column_count:
            arrived = moving = finished
            for to in range(k + 1, column_count):
                moving = lax.ppermute(moving, "cols", [(to - 1, to)])
                arrived = jnp.where(column == to, moving, arrived)
            update = jnp.zeros_like(pending)
            for b in range(side):
                update += times_transposed(arrived[:, b * width : (b + 1) * width], parts[k * side + b])
            pending = pending - jnp.where(k < column, update, jnp.float32(0.0))
    row_sums = lax.psum(jnp.sum(vectors * vectors, axis=1), "cols")
    return (vectors, row_sums / total_width)


def solution(mesh):
    placed = (P("rows", "cols"), P("cols", "rows"), P("cols", None), P(), P("rows"))
    return jax.shard_map(
        per_device,
        mesh=mesh,
        in_specs=placed,
        out_specs=(P("rows", "cols"), P("rows")),
        check_vma=False,
    )
```

```python
import functools
import jax
import jax.numpy as jnp
from jax import lax
from jax.experimental import pallas as pl
from jax.experimental.pallas import tpu as pltpu
from jax.sharding import PartitionSpec as P

MESH = pl.DeviceIdType.MESH


def times_transposed(left, right):
    return lax.dot_general(
        left,
        right,
        (((1,), (1,)), ((), ())),
        precision=lax.Precision.HIGH,
        preferred_element_type=jnp.float32,
    )


def gather_kernel(groups, side, chunks, part_ref, row_ref, mine, in_sem, keep_sem, right_sem, left_sem, hop_sem, side_sem, cross_sem, feed_sem, drop_sem, land_sem):
    row, column = lax.axis_index("rows"), lax.axis_index("cols")
    a, b = row // side, row % side
    depth, width = part_ref.shape
    tall = depth // chunks
    client = groups - 2
    is_client, is_carrier = column == client, column == 0
    needed = jnp.where(is_carrier, client, column)
    partner = jnp.where(is_carrier, client, 0)

    def at(a_to, b_to):
        return (a_to * side + b_to, column)

    barrier = pltpu.get_barrier_semaphore()
    for step in (1, groups - 1):
        pl.semaphore_signal(barrier, inc=1, device_id=at((a + step) % groups, b), device_id_type=MESH)
    for step in range(1, side):
        pl.semaphore_signal(barrier, inc=1, device_id=at(a, (b + step) % side), device_id_type=MESH)

    @pl.when(is_client | is_carrier)
    def _():
        pl.semaphore_signal(barrier, inc=1, device_id=(row, partner), device_id_type=MESH)

    pl.semaphore_wait(barrier, 1 + side + jnp.where(is_client | is_carrier, 1, 0))

    def rows_of(i):
        return pl.ds(pl.multiple_of(i * tall, tall), tall)

    def place(k, b_of, i):
        return row_ref.at[k * side + b_of, rows_of(i), :]

    def right(k, i, source):
        return pltpu.make_async_remote_copy(source, place(k, b, i), right_sem.at[k, i], hop_sem.at[k, i], device_id=at(jnp.minimum(a + 1, groups - 1), b), device_id_type=MESH)

    def left(k, i, source):
        return pltpu.make_async_remote_copy(source, place(k, b, i), left_sem.at[k, i], hop_sem.at[k, i], device_id=at(jnp.maximum(a - 1, 0), b), device_id_type=MESH)

    def across(k, step, i, source):
        return pltpu.make_async_remote_copy(source, place(k, b, i), side_sem.at[step - 1, k, i], cross_sem.at[step - 1, k, i], device_id=at(a, (b + step) % side), device_id_type=MESH)

    def crossed(k, step, i):
        came = place(k, (b + side - step) % side, i)
        return pltpu.make_async_remote_copy(came, came, side_sem.at[step - 1, k, i], cross_sem.at[step - 1, k, i], device_id=at(a, (b + step) % side), device_id_type=MESH)

    def feed(i, source):
        return pltpu.make_async_remote_copy(source, place(a, b, i), feed_sem.at[0, i], feed_sem.at[1, i], device_id=(row, partner), device_id_type=MESH)

    def drop(k, step, i):
        block = place(k, (b + side - step) % side, i)
        return pltpu.make_async_remote_copy(block, block, drop_sem.at[step, k, i], land_sem.at[step, k, i], device_id=(row, partner), device_id_type=MESH)

    def load(i):
        return pltpu.make_async_copy(part_ref.at[rows_of(i), :], mine.at[rows_of(i), :], in_sem.at[i])

    def keep(i):
        return pltpu.make_async_copy(mine.at[rows_of(i), :], place(a, b, i), keep_sem.at[i])

    def by_carrier(k, i):
        return (k == 0) | (i % 3 == 0)

    def cross(k, i, source):
        for step in range(1, side):
            across(k, step, i, source).start()

    def spread(k, i, source):
        @pl.when((k <= a) & (a < groups - 1))
        def _():
            right(k, i, source).start()

        @pl.when((k >= a) & (a > 0))
        def _():
            left(k, i, source).start()

        @pl.when(column > 0)
        def _():
            cross(k, i, source)

        @pl.when(is_carrier)
        def _():
            @pl.when(by_carrier(k, i))
            def _():
                cross(k, i, source)

            @pl.when(k != a)
            def _():
                drop(k, 0, i).start()

    @pl.when((a < column))
    def _():
        @pl.loop(0, chunks)
        def _(i):
            load(i).start()

        @pl.loop(0, chunks)
        def _(i):
            source = mine.at[rows_of(i), :]
            load(i).wait()

            @pl.when(is_client)
            def _():
                feed(i, source).start()

                @pl.when(jnp.logical_not(by_carrier(a, i)))
                def _():
                    cross(a, i, source)

            @pl.when(jnp.logical_not(is_client))
            def _():
                spread(a, i, source)

            keep(i).start()

    @pl.when(is_carrier & (a < client))
    def _():
        @pl.loop(0, chunks)
        def _(i):
            feed(i, place(a, b, i)).wait_recv()
            spread(a, i, place(a, b, i))

    for hop in range(1, groups + 1):
        @pl.loop(0, chunks)
        def _(i):
            if hop < groups:
                for k, towards in ((a - hop, right), (a + hop, left)):
                    @pl.when((k >= 0) & (k < needed))
                    def _():
                        @pl.when(jnp.logical_not(is_client))
                        def _():
                            towards(k, i, place(k, b, i)).wait_recv()
                            spread(k, i, place(k, b, i))

                        @pl.when(is_client)
                        def _():
                            drop(k, 0, i).wait_recv()

                            @pl.when(jnp.logical_not(by_carrier(k, i)))
                            def _():
                                cross(k, i, place(k, b, i))

            for k in (a - hop + 1, a + hop - 1) if hop > 1 else (a,):
                @pl.when(is_carrier & (k >= 0) & (k < needed) & by_carrier(k, i))
                def _():
                    for step in range(1, side):
                        crossed(k, step, i).wait_recv()
                        drop(k, step, i).start()

    for k in range(groups - 1):
        @pl.when(k < needed)
        def _():
            @pl.loop(0, chunks)
            def _(i):
                source = place(k, b, i)

                @pl.when(is_client)
                def _():
                    @pl.when(k == a)
                    def _():
                        feed(i, source).wait_send()

                    for step in range(1, side):
                        @pl.when(by_carrier(k, i))
                        def _():
                            drop(k, step, i).wait_recv()

                        @pl.when(jnp.logical_not(by_carrier(k, i)))
                        def _():
                            crossed(k, step, i).wait_recv()
                            across(k, step, i, source).wait_send()

                @pl.when(jnp.logical_not(is_client))
                def _():
                    @pl.when((k <= a) & (a < groups - 1))
                    def _():
                        right(k, i, source).wait_send()

                    @pl.when((k >= a) & (a > 0))
                    def _():
                        left(k, i, source).wait_send()

                @pl.when((column > 0) & jnp.logical_not(is_client))
                def _():
                    for step in range(1, side):
                        crossed(k, step, i).wait_recv()
                        across(k, step, i, source).wait_send()

                @pl.when(is_carrier)
                def _():
                    @pl.when(k != a)
                    def _():
                        drop(k, 0, i).wait_send()

                    @pl.when(by_carrier(k, i))
                    def _():
                        for step in range(1, side):
                            across(k, step, i, source).wait_send()
                            drop(k, step, i).wait_send()

                @pl.when((k == a) & (column > 0))
                def _():
                    keep(i).wait()


def gather_factor(factor, rows, groups):
    side = rows // groups
    depth, width = factor.shape
    chunks = max(1, depth // 256)
    sem = pltpu.SemaphoreType.DMA
    return pl.pallas_call(
        functools.partial(gather_kernel, groups, side, chunks),
        out_shape=jax.ShapeDtypeStruct(((groups - 1) * side, depth, width), jnp.float32),
        in_specs=[pl.BlockSpec(memory_space=pl.ANY)],
        out_specs=pl.BlockSpec(memory_space=pl.ANY),
        scratch_shapes=[
            pltpu.VMEM((depth, width), jnp.float32),
            sem((chunks,)),
            sem((chunks,)),
            sem((groups, chunks)),
            sem((groups, chunks)),
            sem((groups, chunks)),
            sem((side - 1, groups, chunks)),
            sem((side - 1, groups, chunks)),
            sem((2, chunks)),
            sem((side, groups, chunks)),
            sem((side, groups, chunks)),
        ],
        compiler_params=pltpu.CompilerParams(collective_id=0, has_side_effects=True, vmem_limit_bytes=60000 * 1024),
        cost_estimate=pl.CostEstimate(flops=0, bytes_accessed=600000000, transcendentals=0),
    )(factor)


def per_device(slab, factor, block_inverse, pivot_order, row_count):
    rows_here, block_width = slab.shape
    row_devices = lax.axis_size("rows")
    column_count = lax.axis_size("cols")
    column = lax.axis_index("cols")
    total_width = block_width * column_count
    side = row_devices // column_count
    chosen = lax.dynamic_slice_in_dim(pivot_order, column * block_width, block_width)
    gathered = lax.all_gather(slab, "cols", axis=1, tiled=True)
    parts = gather_factor(factor, row_devices, column_count)
    gathered, parts = lax.optimization_barrier((gathered, parts))
    ordered = jnp.take(gathered, chosen, axis=1)
    live_rows = jnp.arange(rows_here, dtype=jnp.int32) < row_count[0]
    pending = jnp.where(live_rows[:, None], ordered, jnp.float32(0.0))

    width = factor.shape[1]
    vectors = jnp.zeros_like(pending)
    held = []
    for j in range(column_count):
        if j:
            held = [lax.ppermute(block, "cols", [(j - 1, j)]) for block in held + [vectors]]

        def finish(values, *earlier):
            for k, block in enumerate(earlier):
                for b in range(side):
                    values = values - times_transposed(block[:, b * width : (b + 1) * width], parts[k * side + b])
            return times_transposed(values, block_inverse)

        def nothing(values, *earlier):
            return vectors

        vectors = lax.cond(column == j, finish, nothing, pending, *held)
    row_sums = lax.psum(jnp.sum(vectors * vectors, axis=1), "cols")
    return (vectors, row_sums / total_width)


def solution(mesh):
    placed = (P("rows", "cols"), P("cols", "rows"), P("cols", None), P(), P("rows"))
    return jax.shard_map(
        per_device,
        mesh=mesh,
        in_specs=placed,
        out_specs=(P("rows", "cols"), P("rows")),
        check_vma=False,
    )
```
